32 devices in a mesh: member: 4 (over y, core), dp: 4 (over z), tensor: 2 (over x).
Axes of the slice: x: 2, y: 2, z: 4, core: 2. Of those that a mesh axis runs over, the one named last changes fastest.
Arguments:
- context: bfloat16 [2048, 5120], P(('member', 'dp'), 'tensor'), parts along dimension 0, may hold values from -6 to 6
- out_weight: bfloat16 [20480, 5120], P(('member', 'tensor'), 'dp'), parts along dimension 0, may hold values from -0.078125 to 0.078125
- residual: bfloat16 [2048, 5120], P(('member', 'dp', 'tensor')), parts along dimension 0, may hold values from -16 to 16
- norm_gain: float32 [20480], P('member'), parts along dimension 0, may hold values from 0.5 to 1.5
- head_weight: bfloat16 [38016, 5120], P(('member', 'dp', 'tensor')), parts along dimension 0, may hold values from -8 to 8
- targets: int32 [2048], P('member'), parts along dimension 0, may hold values from 0 to 9503
Outputs:
- stream: bfloat16 [2048, 5120], P(('member', 'dp', 'tensor')), parts along dimension 0
- token_loss: float32 [2048], P(('member', 'dp', 'tensor')), parts along dimension 0
The draws below stay inside these ranges and needn't reach their ends.
There are 4 independent parts, one for each index of `member`. The reference program is written for one: setup_inputs(seed, part) draws one part's arguments, and reference() takes and returns one part's arrays. A program takes and returns all parts, laid end to end along the dimension named above; each array names one. Nothing has to cross between parts.
All inputs are finite; a program needn't handle non-finite values.
Results may differ from the reference program's by a relative error of at most 0.001.
Values may be sent and summed in bfloat16 or wider, within the bound.
No kernel may reach another device: no remote copies, remote signals or barrier semaphores. Data moves between devices by JAX's collectives and lax.ppermute only.
A program may use at most 128 MiB of HBM per device.

```python
import math
import jax
import jax.numpy as jnp
import numpy as np
from jax import lax

D = 5120
HQ = 40
HD = 128
VOC_DEV = 1188
TOKENS = 512
VOCAB = 9504
N_DP = 4
N_TENSOR = 2


def directions(key):
    raw = jax.random.normal(jax.random.fold_in(key, 7001), (4, D), jnp.float32)
    return jnp.where(raw >= 0.0, 1.0, -1.0).astype(jnp.float32)


def drawn_tokens():
    table = np.zeros((TOKENS, 4), np.float32)
    for index in range(8):
        table[index * TOKENS // 8 + TOKENS // 16, index % 4] = 6.0
    return jnp.asarray(table)


def drawn_vocab():
    table = np.zeros((VOCAB, 4), np.float32)
    strengths = [120.0, 200.0, 280.0, 360.0]
    for index in range(4):
        first = index * VOCAB // 4 + VOCAB // 8
        table[first, index] = strengths[index]
        table[first + VOCAB // 16, index] = strengths[index] - 2.0
    return jnp.asarray(table / D)


def draw_residual(key, part):
    noise = jax.random.normal(jax.random.fold_in(key, 11), (TOKENS, D), jnp.float32)
    table = drawn_tokens()
    chosen = jnp.sum(table, axis=1, keepdims=True) > 0.0
    aligned = jnp.dot(table, directions(key)) + 0.3 * noise
    other = noise
    values = jnp.where(chosen, aligned, other)
    return jnp.clip(values, -16.0, 16.0).astype(jnp.bfloat16)


def draw_head_weight(key, part):
    scale = 3.0 / math.sqrt(D)
    noise = jax.random.normal(jax.random.fold_in(key, 21), (VOCAB, D), jnp.float32)
    table = drawn_vocab()
    chosen = jnp.sum(table, axis=1, keepdims=True) > 0.0
    aligned = jnp.dot(table, directions(key))
    other = jnp.clip(noise, -6.0, 6.0) * scale
    values = jnp.where(chosen, aligned, other)
    return jnp.clip(values, -8.0, 8.0).astype(jnp.bfloat16)


def set_ends(entries, own_key, low, high):
    place = [jax.random.randint(jax.random.fold_in(own_key, axis), (), 0, length) for axis, length in enumerate(entries.shape)]
    longest = entries.shape.index(max(entries.shape))
    neighbour = place[:longest] + [(place[longest] + 1) % entries.shape[longest]] + place[longest + 1:]
    return entries.at[tuple(place)].set(low).at[tuple(neighbour)].set(high)


def levels(key, dims, shards, smallest, largest):
    gain, own = 1.0, jax.random.fold_in(key, 6)
    for axis_at, shards_of in shards:
        draws = jnp.exp(jax.random.uniform(jax.random.fold_in(own, axis_at), (shards_of,), jnp.float32, smallest / len(shards), largest / len(shards)))
        gain = gain * jnp.repeat(draws, dims[axis_at] // shards_of).reshape([-1 if axis == axis_at else 1 for axis in range(len(dims))])
    return gain


def normal_values(rng, dims, deviation, limit, pieces=(), kind=jnp.bfloat16):
    values = deviation * jax.random.normal(rng, dims, jnp.float32)
    if pieces:
        values = values * levels(rng, dims, pieces, -0.22, 0.18)
    return jnp.clip(values, -limit, limit).astype(kind)


def setup_inputs(seed: int = 0, part: int = 0) -> dict:
    seeds = jax.random.split(jax.random.key(seed), 7)
    part_splits = jax.random.split(jax.random.fold_in(seeds[6], part), 7)
    context = normal_values(part_splits[0], (TOKENS, HQ * HD), 1.0, 6.0, ((0, 4), (1, 2)))
    out_weight = normal_values(part_splits[1], (HQ * HD, D), (HQ * HD) ** -0.5, 0.078125, ((0, 2), (1, 4)))
    residual = draw_residual(jax.random.fold_in(jax.random.fold_in(seeds[6], part), 71), part)
    norm_gain = jnp.clip(1.0 + 0.1 * jax.random.normal(part_splits[3], (D,), jnp.float32), 0.5, 1.5)
    head_weight = draw_head_weight(jax.random.fold_in(jax.random.fold_in(seeds[6], part), 71), part)
    targets = set_ends(jax.random.randint(part_splits[5], (TOKENS,), 0, VOCAB), jax.random.fold_in(part_splits[5], 1), 0, VOCAB - 1).astype(jnp.int32)
    return {"context": context, "out_weight": out_weight, "residual": residual, "norm_gain": norm_gain, "head_weight": head_weight, "targets": targets}


EPSILON = 1e-06

def normalize(stream, norm_gain):
    values = stream.astype(jnp.float32)
    mean_square = lax.optimization_barrier(jnp.mean(values * values, axis=-1, keepdims=True))
    return (values * lax.rsqrt(mean_square + EPSILON) * norm_gain).astype(jnp.bfloat16)

def reference(context, out_weight, residual, norm_gain, head_weight, targets):
    attended = jnp.dot(context, out_weight, preferred_element_type=jnp.float32)
    stream = (residual.astype(jnp.float32) + attended).astype(jnp.bfloat16)
    normed = normalize(stream, norm_gain)
    blocks = head_weight.reshape(N_DP * N_TENSOR, VOC_DEV, D)
    offsets = (jnp.arange(N_DP * N_TENSOR, dtype=jnp.int32) * VOC_DEV).astype(jnp.int32)

    def block_stats(inputs):
        weights, offset = inputs
        logits = lax.dot_general(normed, weights, (((1,), (1,)), ((), ())), preferred_element_type=jnp.float32)
        highest = lax.optimization_barrier(jnp.max(logits, axis=1))
        summed = lax.optimization_barrier(jnp.sum(jnp.exp(logits - highest[:, None]), axis=1))
        columns = jnp.arange(VOC_DEV, dtype=jnp.int32)[None, :] + offset
        picked = lax.optimization_barrier(jnp.sum(jnp.where(columns == targets[:, None], logits, 0.0), axis=1))
        return (highest, summed, picked)
    block_max, block_sum, block_pick = lax.map(block_stats, (blocks, offsets))
    row_max = lax.optimization_barrier(jnp.max(block_max, axis=0))
    row_sum = lax.optimization_barrier(jnp.sum(block_sum * jnp.exp(block_max - row_max[None, :]), axis=0))
    token_loss = jnp.log(row_sum) + row_max - lax.optimization_barrier(jnp.sum(block_pick, axis=0))
    return (stream, token_loss)
```

```python
import functools

import jax
import jax.numpy as jnp
from jax import lax
from jax.experimental import pallas as pl
from jax.experimental.pallas import tpu as pltpu
from jax.sharding import PartitionSpec as P


EPSILON = 1e-06


def halves(local_rows):
    return 2 if local_rows % 64 == 0 else 1


def ahead(value, shift, count):
    moved = value + shift
    return jnp.where(moved >= count, moved - count, moved)


def behind(value, shift, count):
    moved = value - shift
    return jnp.where(moved < 0, moved + count, moved)


def head_kernel(shape, where_ref, wanted_ref, gain_ref, weight_ref, *rest):
    dp_count, tensor_count, rows, columns, vocab = shape
    blocks = rest[: dp_count * tensor_count]
    out_ref, normed_ref = rest[dp_count * tensor_count :]
    step = pl.program_id(0)

    @pl.when(step == 0)
    def _():
        start = where_ref[0]
        for j in range(tensor_count):
            for rho in range(dp_count):
                taken = []
                squares = jnp.zeros((rows, 1), jnp.float32)
                for k in range(dp_count):
                    s = (rho - k) % dp_count
                    value = blocks[j * dp_count + k][s * rows : (s + 1) * rows, :]
                    value = value.astype(jnp.float32)
                    squares = squares + jnp.sum(value * value, axis=1, keepdims=True)
                    taken.append(value)
                scale = lax.rsqrt(squares / (dp_count * columns) + EPSILON)
                first = (j * dp_count + rho) * rows
                for k, value in enumerate(taken):
                    owner = start - k
                    owner = jnp.where(owner < 0, owner + dp_count, owner)
                    at = pl.multiple_of(owner * columns, columns)
                    gain = gain_ref[:, pl.ds(at, columns)]
                    normed_ref[first : first + rows, pl.ds(at, columns)] = (
                        value * scale * gain
                    ).astype(jnp.bfloat16)
        count = out_ref.shape[1]
        out_ref[0:1, :] = jnp.full((1, count), -jnp.inf, jnp.float32)
        out_ref[1:3, :] = jnp.zeros((2, count), jnp.float32)

    logits = lax.dot_general(
        weight_ref[...],
        normed_ref[...],
        (((1,), (1,)), ((), ())),
        preferred_element_type=jnp.float32,
    )
    entry = lax.broadcasted_iota(jnp.int32, logits.shape, 0) + step * logits.shape[0]
    masked = jnp.where(entry < vocab, logits, -jnp.inf)
    before = out_ref[0:1, :]
    highest = jnp.maximum(before, jnp.max(masked, axis=0, keepdims=True))
    out_ref[1:2, :] = out_ref[1:2, :] * jnp.exp(before - highest) + jnp.sum(
        jnp.exp(masked - highest), axis=0, keepdims=True
    )
    out_ref[0:1, :] = highest
    hit = jnp.logical_and(entry == wanted_ref[...], entry < vocab)
    out_ref[2:3, :] = out_ref[2:3, :] + jnp.sum(
        jnp.where(hit, logits, 0.0), axis=0, keepdims=True
    )


def head_stats(blocks, d, wanted, norm_gain, head_weight, shape):
    dp_count, tensor_count, rows, columns, vocab = shape
    count = dp_count * tensor_count * rows
    width = dp_count * columns
    steps = 5
    entries = -(-vocab // (steps * 16)) * 16
    steps = -(-vocab // entries)
    return pl.pallas_call(
        functools.partial(head_kernel, shape),
        grid=(steps,),
        in_specs=[
            pl.BlockSpec(memory_space=pltpu.SMEM),
            pl.BlockSpec((1, count), lambda i: (0, 0)),
            pl.BlockSpec((1, width), lambda i: (0, 0)),
            pl.BlockSpec((entries, width), lambda i: (i, 0)),
        ]
        + [pl.BlockSpec(memory_space=pltpu.VMEM)] * len(blocks),
        out_specs=pl.BlockSpec((3, count), lambda i: (0, 0)),
        out_shape=jax.ShapeDtypeStruct((3, count), jnp.float32),
        scratch_shapes=[pltpu.VMEM((count, width), jnp.bfloat16)],
        compiler_params=pltpu.CompilerParams(
            dimension_semantics=("arbitrary",), vmem_limit_bytes=40 * 1024 * 1024
        ),
        cost_estimate=pl.CostEstimate(
            flops=2 * count * width * vocab,
            bytes_accessed=2 * vocab * width + 4 * count * width,
            transcendentals=count * vocab,
        ),
        name="head_stats",
    )(d.reshape(1), wanted, norm_gain, head_weight, *blocks)


def local(context, out_weight, residual, norm_gain, head_weight, targets):
    dp_count = lax.axis_size("dp")
    tensor_count = lax.axis_size("tensor")
    d = lax.axis_index("dp")
    t = lax.axis_index("tensor")
    local_rows, width = residual.shape
    parts = halves(local_rows)
    rows = local_rows // parts
    depth = context.shape[1]
    columns = out_weight.shape[1]
    vocab = head_weight.shape[0]
    vocab_start = (d * tensor_count + t) * vocab

    def along_dp(value, shift):
        return lax.ppermute(
            value, "dp", [(i, (i + shift) % dp_count) for i in range(dp_count)]
        )

    def along_tensor(value, shift):
        return lax.ppermute(
            value, "tensor", [(i, (i + shift) % tensor_count) for i in range(tensor_count)]
        )

    residuals = []
    for s in range(dp_count):
        cut = lax.dynamic_slice(
            residual, (0, ahead(d, s, dp_count) * columns), (local_rows, columns)
        )
        residuals.append(along_dp(cut, s) if s else cut)

    by_tensor = context.reshape(tensor_count, parts, rows, depth)
    gathered = []
    for h in range(parts):
        held = jnp.concatenate(
            [
                lax.dynamic_index_in_dim(
                    by_tensor[:, h], ahead(t, 1 + j, tensor_count) if j + 1 < tensor_count else t, 0, keepdims=False
                )
                for j in range(tensor_count)
            ],
            axis=0,
        )
        pieces = []
        for s in range(dp_count):
            if s:
                held = along_dp(held, 1)
            partial = jnp.dot(held, out_weight, preferred_element_type=jnp.float32)
            total = partial[(tensor_count - 1) * rows :]
            for j in range(1, tensor_count):
                total = total + along_tensor(partial[(j - 1) * rows : j * rows], j)
            mine = residuals[s][h * rows : (h + 1) * rows]
            if h:
                mine, _ = lax.optimization_barrier((mine, gathered[h - 1][0][0]))
            mine = mine.astype(jnp.float32)
            pieces.append((mine + total).astype(jnp.bfloat16))
        block = jnp.concatenate(pieces, axis=0)
        arrived = []
        for k in range(dp_count):
            if k:
                block = along_dp(block, 1)
            arrived.append([block] + [along_tensor(block, j) for j in range(1, tensor_count)])
        gathered.append(arrived)

    def spread(parts_by_k):
        rows_out = parts_by_k[0].shape[0]
        out = jnp.zeros((rows_out, width), jnp.bfloat16)
        for k, value in enumerate(parts_by_k):
            column = behind(d, k, dp_count) * columns
            out = lax.dynamic_update_slice(out, value, (0, column))
        return out

    def block_rows(block, rho, k):
        s = (rho - k) % dp_count
        return block[s * rows : (s + 1) * rows]

    stream = spread(
        [
            jnp.concatenate([block_rows(gathered[h][k][0], 0, k) for h in range(parts)], axis=0)
            for k in range(dp_count)
        ]
    )

    target_table = targets.reshape(dp_count, tensor_count, parts, rows) - vocab_start
    stats = []
    for h in range(parts):
        wanted = jnp.concatenate(
            [
                target_table[behind(d, rho, dp_count), behind(t, j, tensor_count), h]
                for j in range(tensor_count)
                for rho in range(dp_count)
            ]
        )
        blocks = [gathered[h][k][j] for j in range(tensor_count) for k in range(dp_count)]
        stats.append(
            head_stats(
                blocks,
                d,
                wanted[None, :],
                norm_gain[None, :],
                head_weight,
                (dp_count, tensor_count, rows, columns, vocab),
            )
        )

    table = jnp.stack(stats).reshape(parts, 3, tensor_count, dp_count, rows)
    table = jnp.transpose(table, (3, 2, 1, 0, 4)).reshape(
        dp_count, tensor_count, 3, local_rows
    )
    table = jnp.take(table, behind(d, jnp.arange(dp_count), dp_count), axis=0)
    table = jnp.take(
        table, behind(t, jnp.arange(tensor_count), tensor_count), axis=1
    )
    table = table.reshape(dp_count * tensor_count, 3, local_rows)
    table = lax.all_to_all(table, ("dp", "tensor"), 0, 0, tiled=True)
    row_max = jnp.max(table[:, 0], axis=0)
    row_sum = jnp.sum(table[:, 1] * jnp.exp(table[:, 0] - row_max[None]), axis=0)
    token_loss = jnp.log(row_sum) + row_max - jnp.sum(table[:, 2], axis=0)
    return (stream, token_loss)


def solution(mesh):
    def program(context, out_weight, residual, norm_gain, head_weight, targets):
        step = jax.shard_map(
            local,
            mesh=mesh,
            in_specs=(
                P(("member", "dp"), "tensor"),
                P(("member", "tensor"), "dp"),
                P(("member", "dp", "tensor"), None),
                P("member"),
                P(("member", "dp", "tensor"), None),
                P("member"),
            ),
            out_specs=(P(("member", "dp", "tensor"), None), P(("member", "dp", "tensor"))),
            check_vma=False,
        )
        return step(context, out_weight, residual, norm_gain, head_weight, targets)

    return program
```

```python
import functools

import jax
import jax.numpy as jnp
from jax import lax
from jax.experimental import pallas as pl
from jax.experimental.pallas import tpu as pltpu
from jax.sharding import PartitionSpec as P


EPSILON = 1e-06
VMEM = pl.BlockSpec(memory_space=pltpu.VMEM)
SMEM = pl.BlockSpec(memory_space=pltpu.SMEM)


def halves(local_rows):
    return 2 if local_rows % 64 == 0 else 1


def ahead(value, shift, count):
    moved = value + shift
    return jnp.where(moved >= count, moved - count, moved)


def behind(value, shift, count):
    moved = value - shift
    return jnp.where(moved < 0, moved + count, moved)


def stream_kernel(shape, part, where_ref, *refs):
    dp_count, tensor_count, rows = shape
    partials, refs = refs[:dp_count], refs[dp_count:]
    residuals, refs = refs[:dp_count], refs[dp_count:]
    received, out_ref = refs[:-1], refs[-1]
    first = pl.multiple_of(where_ref[1] * rows, rows)
    for s in range(dp_count):
        total = partials[s][pl.ds(first, rows), :]
        for j in range(tensor_count - 1):
            total = total + received[s * (tensor_count - 1) + j][...]
        mine = residuals[s][part * rows : (part + 1) * rows, :].astype(jnp.float32)
        out_ref[s * rows : (s + 1) * rows, :] = (mine + total).astype(jnp.bfloat16)


def stream_block(where, partials, residuals, received, shape, part):
    dp_count, _, rows = shape
    columns = residuals[0].shape[1]
    return pl.pallas_call(
        functools.partial(stream_kernel, shape, part),
        in_specs=[SMEM] + [VMEM] * (2 * dp_count + len(received)),
        out_specs=VMEM,
        out_shape=jax.ShapeDtypeStruct((dp_count * rows, columns), jnp.bfloat16),
        compiler_params=pltpu.CompilerParams(vmem_limit_bytes=16 * 1024 * 1024),
        cost_estimate=pl.CostEstimate(
            flops=100_000_000, bytes_accessed=12 * dp_count * rows * columns, transcendentals=0
        ),
    )(where, *partials, *residuals, *received)


def head_kernel(shape, where_ref, wanted_ref, earlier_ref, gain_ref, weight_ref, *rest):
    dp_count, tensor_count, rows, columns, vocab, part = shape
    devices = dp_count * tensor_count
    blocks = rest[:devices]
    out_ref, normed_ref, stats_ref = rest[devices:]
    step = pl.program_id(0)

    @pl.when(step == 0)
    def _():
        for j in range(tensor_count):
            tensor = behind(where_ref[1], j, tensor_count)
            for rho in range(dp_count):
                taken = []
                squares = jnp.zeros((rows, 1), jnp.float32)
                for k in range(dp_count):
                    s = (rho - k) % dp_count
                    value = blocks[j * dp_count + k][s * rows : (s + 1) * rows, :]
                    value = value.astype(jnp.float32)
                    squares = squares + jnp.sum(value * value, axis=1, keepdims=True)
                    taken.append(value)
                scale = lax.rsqrt(squares / (dp_count * columns) + EPSILON)
                owner = behind(where_ref[0], rho, dp_count) * tensor_count + tensor
                first = pl.multiple_of(owner * rows, rows)
                for k, value in enumerate(taken):
                    at = pl.multiple_of(behind(where_ref[0], k, dp_count) * columns, columns)
                    gain = gain_ref[:, pl.ds(at, columns)]
                    normed_ref[pl.ds(first, rows), pl.ds(at, columns)] = (
                        value * scale * gain
                    ).astype(jnp.bfloat16)
        count = devices * rows
        stats_ref[0:1, :] = jnp.full((1, count), -jnp.inf, jnp.float32)
        stats_ref[1:3, :] = jnp.zeros((2, count), jnp.float32)

    logits = lax.dot_general(
        weight_ref[...],
        normed_ref[...],
        (((1,), (1,)), ((), ())),
        preferred_element_type=jnp.float32,
    )
    entry = lax.broadcasted_iota(jnp.int32, logits.shape, 0) + step * logits.shape[0]
    masked = jnp.where(entry < vocab, logits, -jnp.inf)
    before = stats_ref[0:1, :]
    highest = jnp.maximum(before, jnp.max(masked, axis=0, keepdims=True))
    stats_ref[1:2, :] = stats_ref[1:2, :] * jnp.exp(before - highest) + jnp.sum(
        jnp.exp(masked - highest), axis=0, keepdims=True
    )
    stats_ref[0:1, :] = highest
    hit = jnp.logical_and(entry == wanted_ref[...], entry < vocab)
    stats_ref[2:3, :] = stats_ref[2:3, :] + jnp.sum(
        jnp.where(hit, logits, 0.0), axis=0, keepdims=True
    )

    @pl.when(step == pl.num_programs(0) - 1)
    def _():
        done = 3 * rows * part
        if part:
            out_ref[:, :, :done] = earlier_ref[...]
        for owner in range(devices):
            for item in range(3):
                out_ref[owner, :, done + item * rows : done + (item + 1) * rows] = stats_ref[
                    item : item + 1, owner * rows : (owner + 1) * rows
                ]


def head_stats(blocks, where, wanted, earlier, norm_gain, head_weight, shape):
    dp_count, tensor_count, rows, columns, vocab, part = shape
    devices = dp_count * tensor_count
    count = devices * rows
    width = dp_count * columns
    entries = -(-vocab // (5 * 16)) * 16
    steps = -(-vocab // entries)
    return pl.pallas_call(
        functools.partial(head_kernel, shape),
        grid=(steps,),
        in_specs=[
            SMEM,
            pl.BlockSpec((1, count), lambda i: (0, 0)),
            VMEM,
            pl.BlockSpec((1, width), lambda i: (0, 0)),
            pl.BlockSpec((entries, width), lambda i: (i, 0)),
        ]
        + [VMEM] * len(blocks),
        out_specs=VMEM,
        out_shape=jax.ShapeDtypeStruct((devices, 1, 3 * rows * (part + 1)), jnp.float32),
        scratch_shapes=[
            pltpu.VMEM((count, width), jnp.bfloat16),
            pltpu.VMEM((8, count), jnp.float32),
        ],
        compiler_params=pltpu.CompilerParams(
            dimension_semantics=("arbitrary",), vmem_limit_bytes=40 * 1024 * 1024
        ),
        cost_estimate=pl.CostEstimate(
            flops=2 * count * width * vocab,
            bytes_accessed=2 * vocab * width + 4 * count * width,
            transcendentals=count * vocab,
        ),
    )(where, wanted, earlier, norm_gain, head_weight, *blocks)


def loss_kernel(rows, parts, table_ref, out_ref):
    for h in range(parts):
        base = 3 * rows * h
        highest = table_ref[:, 0, base : base + rows]
        summed = table_ref[:, 0, base + rows : base + 2 * rows]
        picked = table_ref[:, 0, base + 2 * rows : base + 3 * rows]
        top = jnp.max(highest, axis=0, keepdims=True)
        total = jnp.sum(summed * jnp.exp(highest - top), axis=0, keepdims=True)
        loss = jnp.log(total) + top - jnp.sum(picked, axis=0, keepdims=True)
        out_ref[:, rows * h : rows * (h + 1)] = loss


def local(context, out_weight, residual, norm_gain, head_weight, targets):
    dp_count = lax.axis_size("dp")
    tensor_count = lax.axis_size("tensor")
    d = lax.axis_index("dp")
    t = lax.axis_index("tensor")
    where = jnp.stack([d, t]).astype(jnp.int32)
    local_rows, width = residual.shape
    parts = halves(local_rows)
    rows = local_rows // parts
    depth = context.shape[1]
    columns = out_weight.shape[1]
    vocab = head_weight.shape[0]
    devices = dp_count * tensor_count
    vocab_start = (d * tensor_count + t) * vocab

    def along_dp(value, shift):
        return lax.ppermute(
            value, "dp", [(i, (i + shift) % dp_count) for i in range(dp_count)]
        )

    def along_tensor(value, shift):
        return lax.ppermute(
            value, "tensor", [(i, (i + shift) % tensor_count) for i in range(tensor_count)]
        )

    residuals = []
    for s in range(dp_count):
        cut = lax.dynamic_slice(
            residual, (0, ahead(d, s, dp_count) * columns), (local_rows, columns)
        )
        residuals.append(along_dp(cut, s) if s else cut)

    by_tensor = context.reshape(tensor_count, parts, rows, depth)
    shape = (dp_count, tensor_count, rows)
    gathered = []
    for h in range(parts):
        held = by_tensor[:, h].reshape(tensor_count * rows, depth)
        partials, received = [], []
        for s in range(dp_count):
            if s:
                held = along_dp(held, 1)
            partial = jnp.dot(held, out_weight, preferred_element_type=jnp.float32)
            partials.append(partial)
            for j in range(1, tensor_count):
                other = lax.dynamic_slice(
                    partial, (ahead(t, j, tensor_count) * rows, 0), (rows, columns)
                )
                received.append(along_tensor(other, j))
        block = stream_block(where, partials, residuals, received, shape, h)
        arrived = []
        for k in range(dp_count):
            if k:
                block = along_dp(block, 1)
            if h == parts - 1 and k == dp_count - 1:
                others = [along_dp(arrived[-1][j], 1) for j in range(1, tensor_count)]
            else:
                others = [along_tensor(block, j) for j in range(1, tensor_count)]
            arrived.append([block] + others)
        gathered.append(arrived)

    stream = jnp.zeros((local_rows, width), jnp.bfloat16)
    for k in range(dp_count):
        s = (dp_count - k) % dp_count
        piece = jnp.concatenate(
            [gathered[h][k][0][s * rows : (s + 1) * rows] for h in range(parts)], axis=0
        )
        stream = lax.dynamic_update_slice(stream, piece, (0, behind(d, k, dp_count) * columns))

    wanted = targets.reshape(devices, parts, rows) - vocab_start
    table = jnp.zeros((devices, 1, 128), jnp.float32)
    for h in range(parts):
        blocks = [gathered[h][k][j] for j in range(tensor_count) for k in range(dp_count)]
        table = head_stats(
            blocks,
            where,
            wanted[:, h].reshape(1, devices * rows),
            table,
            norm_gain[None, :],
            head_weight,
            (dp_count, tensor_count, rows, columns, vocab, h),
        )

    table = lax.all_to_all(table, ("dp", "tensor"), 0, 0, tiled=True)
    token_loss = pl.pallas_call(
        functools.partial(loss_kernel, rows, parts),
        in_specs=[VMEM],
        out_specs=VMEM,
        out_shape=jax.ShapeDtypeStruct((1, local_rows), jnp.float32),
        compiler_params=pltpu.CompilerParams(vmem_limit_bytes=4 * 1024 * 1024),
        name="loss",
    )(table).reshape(local_rows)
    return (stream, token_loss)


def solution(mesh):
    def program(context, out_weight, residual, norm_gain, head_weight, targets):
        step = jax.shard_map(
            local,
            mesh=mesh,
            in_specs=(
                P(("member", "dp"), "tensor"),
                P(("member", "tensor"), "dp"),
                P(("member", "dp", "tensor"), None),
                P("member"),
                P(("member", "dp", "tensor"), None),
                P("member"),
            ),
            out_specs=(P(("member", "dp", "tensor"), None), P(("member", "dp", "tensor"))),
            check_vma=False,
        )
        return step(context, out_weight, residual, norm_gain, head_weight, targets)

    return program
```

```python
import functools

import jax
import jax.numpy as jnp
from jax import lax
from jax.experimental import pallas as pl
from jax.experimental.pallas import tpu as pltpu
from jax.sharding import PartitionSpec as P


EPSILON = 1e-06
VMEM = pl.BlockSpec(memory_space=pltpu.VMEM)
SMEM = pl.BlockSpec(memory_space=pltpu.SMEM)


def halves(local_rows):
    return 2 if local_rows % 64 == 0 else 1


def ahead(value, shift, count):
    moved = value + shift
    return jnp.where(moved >= count, moved - count, moved)


def behind(value, shift, count):
    moved = value - shift
    return jnp.where(moved < 0, moved + count, moved)


def stream_kernel(shape, part, where_ref, *refs):
    dp_count, tensor_count, rows = shape
    partials, refs = refs[:dp_count], refs[dp_count:]
    residuals, refs = refs[:dp_count], refs[dp_count:]
    received, out_ref = refs[:-1], refs[-1]
    first = pl.multiple_of(where_ref[1] * rows, rows)
    for s in range(dp_count):
        total = partials[s][pl.ds(first, rows), :]
        for j in range(tensor_count - 1):
            total = total + received[s * (tensor_count - 1) + j][...]
        mine = residuals[s][part * rows : (part + 1) * rows, :].astype(jnp.float32)
        out_ref[s * rows : (s + 1) * rows, :] = (mine + total).astype(jnp.bfloat16)


def stream_block(where, partials, residuals, received, shape, part):
    dp_count, _, rows = shape
    columns = residuals[0].shape[1]
    return pl.pallas_call(
        functools.partial(stream_kernel, shape, part),
        in_specs=[SMEM] + [VMEM] * (2 * dp_count + len(received)),
        out_specs=VMEM,
        out_shape=jax.ShapeDtypeStruct((dp_count * rows, columns), jnp.bfloat16),
        compiler_params=pltpu.CompilerParams(vmem_limit_bytes=16 * 1024 * 1024),
        cost_estimate=pl.CostEstimate(
            flops=100_000_000, bytes_accessed=12 * dp_count * rows * columns, transcendentals=0
        ),
    )(where, *partials, *residuals, *received)


def scaled_logits(shape, steps, where_ref, gain_ref, weight_ref, blocks, held_ref, square_ref):
    dp_count, tensor_count, rows, columns = shape
    logits = None
    for place, k in enumerate(steps):
        column = pl.multiple_of(behind(where_ref[0], k, dp_count) * columns, columns)
        gain = gain_ref[:, pl.ds(column, columns)]
        for j in range(tensor_count):
            block = blocks[place * tensor_count + j]
            for s in range(dp_count):
                first = (j * dp_count + (k + s) % dp_count) * rows
                value = block[s * rows : (s + 1) * rows, :].astype(jnp.float32)
                total = jnp.broadcast_to(
                    jnp.sum(value * value, axis=1, keepdims=True), (rows, square_ref.shape[1])
                )
                if place:
                    total = total + square_ref[first : first + rows, :]
                square_ref[first : first + rows, :] = total
                held_ref[place, first : first + rows, :] = (value * gain).astype(jnp.bfloat16)
        product = lax.dot_general(
            weight_ref[:, pl.ds(column, columns)],
            held_ref[place],
            (((1,), (1,)), ((), ())),
            preferred_element_type=jnp.float32,
        )
        logits = product if logits is None else logits + product
    return logits


def early_kernel(shape, where_ref, gain_ref, weight_ref, *rest):
    dp_count, tensor_count = shape[:2]
    steps = range(dp_count - 1)
    count = tensor_count * len(steps)
    logits_ref, square_ref, held_ref = rest[count:]
    logits_ref[...] = scaled_logits(
        shape, steps, where_ref, gain_ref, weight_ref, rest[:count], held_ref, square_ref
    )


def final_kernel(shape, part, where_ref, gain_ref, weight_ref, logits_ref, early_ref, *rest):
    wanted_ref, *rest = rest
    if part:
        earlier_ref, *rest = rest
    dp_count, tensor_count, rows, columns = shape
    out_ref, held_ref, square_ref = rest[tensor_count:]
    logits = logits_ref[...] + scaled_logits(
        shape,
        [dp_count - 1],
        where_ref,
        gain_ref,
        weight_ref,
        rest[:tensor_count],
        held_ref,
        square_ref,
    )
    squares = jnp.transpose(early_ref[...] + square_ref[...])[0:1, :]
    logits = logits * lax.rsqrt(squares / (dp_count * columns) + EPSILON)
    entry = lax.broadcasted_iota(jnp.int32, logits.shape, 0)
    owners = [
        behind(where_ref[0], rho, dp_count) * tensor_count + behind(where_ref[1], j, tensor_count)
        for j in range(tensor_count)
        for rho in range(dp_count)
    ]
    wanted = jnp.concatenate(
        [wanted_ref[owner, :, part * rows : (part + 1) * rows] for owner in owners], axis=1
    )
    wanted = wanted - (where_ref[0] * tensor_count + where_ref[1]) * weight_ref.shape[0]
    highest = jnp.max(logits, axis=0, keepdims=True)
    summed = jnp.sum(jnp.exp(logits - highest), axis=0, keepdims=True)
    picked = jnp.sum(
        jnp.where(entry == wanted, logits, 0.0), axis=0, keepdims=True
    )
    done = 3 * rows * part
    if part:
        out_ref[:, :, :done] = earlier_ref[...]
    for place, owner in enumerate(owners):
        for item, value in enumerate((highest, summed, picked)):
            out_ref[owner, :, done + item * rows : done + (item + 1) * rows] = value[
                :, place * rows : (place + 1) * rows
            ]


def head_memory(tokens):
    return (12 if tokens <= 256 else 60) * 1024 * 1024


def head_early(blocks, where, norm_gain, weight, shape):
    dp_count, tensor_count, rows, columns = shape
    count = dp_count * tensor_count * rows
    vocab = weight.shape[0]
    return pl.pallas_call(
        functools.partial(early_kernel, shape),
        in_specs=[SMEM] + [VMEM] * (2 + len(blocks)),
        out_specs=[VMEM, VMEM],
        out_shape=[
            jax.ShapeDtypeStruct((vocab, count), jnp.float32),
            jax.ShapeDtypeStruct((count, 128), jnp.float32),
        ],
        scratch_shapes=[pltpu.VMEM((dp_count - 1, count, columns), jnp.bfloat16)],
        compiler_params=pltpu.CompilerParams(vmem_limit_bytes=head_memory(count)),
        cost_estimate=pl.CostEstimate(
            flops=2 * count * columns * (dp_count - 1) * vocab,
            bytes_accessed=2 * vocab * columns * (dp_count - 1),
            transcendentals=0,
        ),
    )(where, norm_gain, weight, *blocks)


def head_final(blocks, where, norm_gain, weight, logits, squares, wanted, earlier, shape, part):
    dp_count, tensor_count, rows, columns = shape
    devices = dp_count * tensor_count
    count = devices * rows
    vocab = weight.shape[0]
    return pl.pallas_call(
        functools.partial(final_kernel, shape, part),
        in_specs=[SMEM] + [VMEM] * (5 + len(blocks) + (part > 0)),
        out_specs=VMEM,
        out_shape=jax.ShapeDtypeStruct((devices, 1, 3 * rows * (part + 1)), jnp.float32),
        scratch_shapes=[
            pltpu.VMEM((1, count, columns), jnp.bfloat16),
            pltpu.VMEM((count, 128), jnp.float32),
        ],
        compiler_params=pltpu.CompilerParams(vmem_limit_bytes=head_memory(count)),
        cost_estimate=pl.CostEstimate(
            flops=2 * count * columns * vocab,
            bytes_accessed=2 * vocab * columns,
            transcendentals=count * vocab,
        ),
    )(where, norm_gain, weight, logits, squares, wanted, *([earlier] if part else []), *blocks)


def stream_out_kernel(shape, where_ref, *refs):
    dp_count, parts, rows, columns = shape
    out_ref = refs[-1]
    for h in range(parts):
        for k in range(dp_count):
            s = (dp_count - k) % dp_count
            at = pl.multiple_of(behind(where_ref[0], k, dp_count) * columns, columns)
            out_ref[h * rows : (h + 1) * rows, pl.ds(at, columns)] = refs[h * dp_count + k][
                s * rows : (s + 1) * rows, :
            ]


def stream_out(where, blocks, shape):
    dp_count, parts, rows, columns = shape
    return pl.pallas_call(
        functools.partial(stream_out_kernel, shape),
        in_specs=[SMEM] + [VMEM] * len(blocks),
        out_specs=VMEM,
        out_shape=jax.ShapeDtypeStruct((parts * rows, dp_count * columns), jnp.bfloat16),
        compiler_params=pltpu.CompilerParams(vmem_limit_bytes=8 * 1024 * 1024),
        cost_estimate=pl.CostEstimate(
            flops=1_000_000, bytes_accessed=4 * parts * rows * dp_count * columns, transcendentals=0
        ),
        name="stream_out",
    )(where, *blocks)


def loss_kernel(rows, parts, table_ref, out_ref):
    for h in range(parts):
        base = 3 * rows * h
        highest = table_ref[:, 0, base : base + rows]
        summed = table_ref[:, 0, base + rows : base + 2 * rows]
        picked = table_ref[:, 0, base + 2 * rows : base + 3 * rows]
        top = jnp.max(highest, axis=0, keepdims=True)
        total = jnp.sum(summed * jnp.exp(highest - top), axis=0, keepdims=True)
        loss = jnp.log(total) + top - jnp.sum(picked, axis=0, keepdims=True)
        out_ref[:, rows * h : rows * (h + 1)] = loss


def local(context, out_weight, residual, norm_gain, head_weight, targets):
    dp_count = lax.axis_size("dp")
    tensor_count = lax.axis_size("tensor")
    d = lax.axis_index("dp")
    t = lax.axis_index("tensor")
    where = jnp.stack([d, t]).astype(jnp.int32)
    local_rows, _ = residual.shape
    parts = halves(local_rows)
    rows = local_rows // parts
    depth = context.shape[1]
    columns = out_weight.shape[1]
    devices = dp_count * tensor_count

    def along_dp(value, shift):
        return lax.ppermute(
            value, "dp", [(i, (i + shift) % dp_count) for i in range(dp_count)]
        )

    def along_tensor(value, shift):
        return lax.ppermute(
            value, "tensor", [(i, (i + shift) % tensor_count) for i in range(tensor_count)]
        )

    residuals = []
    for s in range(dp_count):
        cut = lax.dynamic_slice(
            residual, (0, ahead(d, s, dp_count) * columns), (local_rows, columns)
        )
        residuals.append(along_dp(cut, s) if s else cut)

    shape = (dp_count, tensor_count, rows)
    gathered = []
    for h in range(parts):
        taken, _ = lax.optimization_barrier((context, where)) if h else (context, where)
        by_tensor = taken.reshape(tensor_count, parts, rows, depth)
        held = by_tensor[:, h].reshape(tensor_count * rows, depth)
        partials, received = [], []
        for s in range(dp_count):
            if s:
                held = along_dp(held, 1)
            partial = jnp.dot(held, out_weight, preferred_element_type=jnp.float32)
            partials.append(partial)
            for j in range(1, tensor_count):
                other = lax.dynamic_slice(
                    partial, (ahead(t, j, tensor_count) * rows, 0), (rows, columns)
                )
                received.append(along_tensor(other, j))
        block = stream_block(where, partials, residuals, received, shape, h)
        arrived = []
        for k in range(dp_count):
            if k:
                block = along_dp(block, 1)
            if h == parts - 1 and k == dp_count - 1:
                others = [along_dp(arrived[-1][j], 1) for j in range(1, tensor_count)]
            else:
                others = [along_tensor(block, j) for j in range(1, tensor_count)]
            arrived.append([block] + others)
        gathered.append(arrived)

    stream = stream_out(
        where,
        [gathered[h][k][0] for h in range(parts) for k in range(dp_count)],
        (dp_count, parts, rows, columns),
    )

    owned = targets.reshape(devices, 1, local_rows)
    table = None
    shape = (dp_count, tensor_count, rows, columns)
    early = []
    for h in range(parts):
        blocks = [block for arrived in gathered[h][:-1] for block in arrived]
        early.append(head_early(blocks, where, norm_gain[None, :], head_weight, shape))
    for h in range(parts):
        table = head_final(
            gathered[h][-1],
            where,
            norm_gain[None, :],
            head_weight,
            *early[h],
            owned,
            table,
            shape,
            h,
        )

    table = lax.all_to_all(table, ("dp", "tensor"), 0, 0, tiled=True)
    token_loss = pl.pallas_call(
        functools.partial(loss_kernel, rows, parts),
        in_specs=[VMEM],
        out_specs=VMEM,
        out_shape=jax.ShapeDtypeStruct((1, local_rows), jnp.float32),
        compiler_params=pltpu.CompilerParams(vmem_limit_bytes=4 * 1024 * 1024),
        name="loss",
    )(table).reshape(local_rows)
    return (stream, token_loss)


def solution(mesh):
    def program(context, out_weight, residual, norm_gain, head_weight, targets):
        step = jax.shard_map(
            local,
            mesh=mesh,
            in_specs=(
                P(("member", "dp"), "tensor"),
                P(("member", "tensor"), "dp"),
                P(("member", "dp", "tensor"), None),
                P("member"),
                P(("member", "dp", "tensor"), None),
                P("member"),
            ),
            out_specs=(P(("member", "dp", "tensor"), None), P(("member", "dp", "tensor"))),
            check_vma=False,
        )
        return step(context, out_weight, residual, norm_gain, head_weight, targets)

    return program
```
